32 devices in a mesh: dp: 8 (over z, y), tp: 4 (over x, core).
Axes of the slice: x: 2, y: 2, z: 4, core: 2. Of those that a mesh axis runs over, the one named last changes fastest.
Arguments:
- hidden: bfloat16 [32, 384, 768], P('dp')
- table: bfloat16 [52224, 768], P('tp')
- labels: int32 [32, 384], P('dp')
- loss_mask: int32 [32, 384], P('dp')
- ln_gain: bfloat16 [768], replicated
- ln_bias: bfloat16 [768], replicated
Outputs:
- output 1: float32 [], replicated
- output 2: bfloat16 [32, 384, 768], P('dp')
- output 3: float32 [52224, 768], P('tp')
- output 4: float32 [768], replicated
- output 5: float32 [768], replicated
All inputs are finite; a program needn't handle non-finite values.
Results may differ from the reference program's by a relative error of at most 0.001.
Values sent between devices are 32-bit elements.
A program may use at most 1 GiB of HBM per device.

```python
import jax
import jax.numpy as jnp
from jax import lax

GROUP_BATCH = 4
DP_GROUPS = 8
SEQ_LEN = 384
MODEL_WIDTH = 768
VOCAB_SIZE = 51865
VOCAB_PAD = 52224
BATCH_SIZE = DP_GROUPS * GROUP_BATCH
LN_EPS = 1e-5


def draw_targets(base_key):
    k_lab, k_grp, k_len, k_pre = jax.random.split(base_key, 4)
    labels = jax.random.randint(k_lab, (BATCH_SIZE, SEQ_LEN), 0, VOCAB_SIZE, dtype=jnp.int32)
    labels = labels.at[0, 0].set(0).at[0, 1].set(VOCAB_SIZE - 1)
    group_top = jax.random.randint(k_grp, (DP_GROUPS,), SEQ_LEN // 8, SEQ_LEN + 1, dtype=jnp.int32)
    seq_top = jnp.repeat(group_top, GROUP_BATCH)
    span_len = seq_top - seq_top // 2 + 1
    lengths = seq_top // 2 + jax.random.randint(k_len, (BATCH_SIZE,), 0, 1 << 20, dtype=jnp.int32) % span_len
    prefix = jax.random.randint(k_pre, (BATCH_SIZE,), 1, SEQ_LEN // 8 + 1, dtype=jnp.int32)
    lengths = jnp.maximum(lengths, prefix + 1)
    positions = jnp.arange(SEQ_LEN, dtype=jnp.int32)[None, :]
    loss_mask = ((positions >= prefix[:, None]) & (positions < lengths[:, None])).astype(jnp.int32)
    return labels, loss_mask


def setup_inputs(seed: int = 0) -> dict:
    base_key = jax.random.key(seed)
    k_hid, k_tab, k_gain, k_bias, k_tgt = jax.random.split(base_key, 5)
    hidden = jax.random.normal(k_hid, (BATCH_SIZE, SEQ_LEN, MODEL_WIDTH), jnp.float32)
    live_rows = (jnp.arange(VOCAB_PAD) < VOCAB_SIZE)[:, None]
    table = jax.random.normal(k_tab, (VOCAB_PAD, MODEL_WIDTH), jnp.float32) * (2.0 * MODEL_WIDTH ** -0.5)
    table = jnp.where(live_rows, table, 0.0)
    ln_gain = 1.0 + 0.3 * jax.random.normal(k_gain, (MODEL_WIDTH,), jnp.float32)
    ln_bias = 0.3 * jax.random.normal(k_bias, (MODEL_WIDTH,), jnp.float32)
    labels, loss_mask = draw_targets(k_tgt)
    return dict(hidden=hidden.astype(jnp.bfloat16), table=table.astype(jnp.bfloat16), labels=labels, loss_mask=loss_mask, ln_gain=ln_gain.astype(jnp.bfloat16), ln_bias=ln_bias.astype(jnp.bfloat16))


def reference(hidden, table, labels, loss_mask, ln_gain, ln_bias):
    count = jnp.sum(loss_mask).astype(jnp.float32)
    gain32 = ln_gain.astype(jnp.float32)
    bias32 = ln_bias.astype(jnp.float32)
    vocab_ids = jnp.arange(VOCAB_PAD)
    valid_cols = (vocab_ids < VOCAB_SIZE)[None, :]

    def one_seq(carry, inputs):
        grad_table, loss_sum = carry
        h_seq, lab_seq, mask_seq = inputs
        h32 = h_seq.astype(jnp.float32)
        mean = jnp.mean(h32, axis=-1, keepdims=True)
        centred = h32 - mean
        variance = jnp.mean(centred * centred, axis=-1, keepdims=True)
        inv_std = lax.rsqrt(variance + LN_EPS)
        x_hat = centred * inv_std
        x_norm = (x_hat * gain32 + bias32).astype(jnp.bfloat16)
        logits = jnp.dot(x_norm, table.T, preferred_element_type=jnp.float32)
        logits = jnp.where(valid_cols, logits, -jnp.inf)
        top = jnp.max(logits, axis=-1, keepdims=True)
        log_norm = top[:, 0] + jnp.log(jnp.sum(jnp.exp(logits - top), axis=-1))
        one_hot = vocab_ids[None, :] == lab_seq[:, None]
        target = jnp.sum(jnp.where(one_hot, logits, 0.0), axis=-1)
        weight = mask_seq.astype(jnp.float32)
        loss_sum = loss_sum + jnp.sum(weight * (log_norm - target))
        prob_vals = jnp.exp(logits - log_norm[:, None])
        grad_logits = ((prob_vals - one_hot.astype(jnp.float32)) * (weight / count)[:, None]).astype(jnp.bfloat16)
        grad_x = jnp.dot(grad_logits, table, preferred_element_type=jnp.float32)
        grad_table = grad_table + jnp.dot(grad_logits.T, x_norm, preferred_element_type=jnp.float32)
        grad_hat = grad_x * gain32
        mean_grad = jnp.mean(grad_hat, axis=-1, keepdims=True)
        mean_proj = jnp.mean(grad_hat * x_hat, axis=-1, keepdims=True)
        grad_h = (inv_std * (grad_hat - mean_grad - x_hat * mean_proj)).astype(jnp.bfloat16)
        return (grad_table, loss_sum), (grad_h, jnp.sum(grad_x * x_hat, axis=0), jnp.sum(grad_x, axis=0))

    init = (jnp.zeros((VOCAB_PAD, MODEL_WIDTH), jnp.float32), jnp.zeros((), jnp.float32))
    (grad_table, loss_sum), (grad_hidden, gain_parts, bias_parts) = lax.scan(one_seq, init, (hidden, labels, loss_mask))
    return loss_sum / count, grad_hidden, grad_table, jnp.sum(gain_parts, axis=0), jnp.sum(bias_parts, axis=0)
```

```python
import functools

import jax
import jax.numpy as jnp
from jax import lax
from jax.experimental import pallas as pl
from jax.experimental.pallas import tpu as pltpu
from jax.sharding import PartitionSpec as P

LN_EPS = 1e-5
VOCAB = 51865
LOG2E = 1.4426950408889634
LOW = -3.0e38
TB = 256
F32 = jnp.float32
BF16 = jnp.bfloat16
VMEM_MAX = 67043328


def nt(a, b):
    return lax.dot_general(a, b, (((1,), (1,)), ((), ())), preferred_element_type=F32)


def nn(a, b):
    return jnp.dot(a, b, preferred_element_type=F32)


def normed(h32):
    mean = jnp.mean(h32, axis=-1, keepdims=True)
    centred = h32 - mean
    variance = jnp.mean(centred * centred, axis=-1, keepdims=True)
    inv_std = lax.rsqrt(variance + LN_EPS)
    return centred * inv_std, inv_std


def prep_kernel(cnt_ref, h_ref, my_ref, g_ref, b_ref, hc_ref, x_ref, pos_ref, yc_ref):
    tokens, width = h_ref.shape
    mask = my_ref[0:1, :]
    live = mask > 0.0
    mrows = jnp.broadcast_to(mask, (8, tokens)).astype(BF16)
    y = my_ref[1:2, :]
    hi = jnp.floor(y * (1.0 / 256.0))
    lo = y - 256.0 * hi
    row8 = lax.broadcasted_iota(jnp.int32, (8, tokens), 0)
    table = jnp.where(row8 == 0, hi, jnp.where(row8 == 1, lo, 1.0)).astype(BF16)
    for i in range(0, tokens, TB):
        src = lax.broadcasted_iota(jnp.int32, (tokens, TB), 0)
        dst = lax.broadcasted_iota(jnp.int32, (tokens, TB), 1) + i
        tri = jnp.where(src <= dst, 1.0, 0.0).astype(BF16)
        pos_ref[:, i : i + TB] = nn(mrows, tri)
    pos = jnp.where(live, pos_ref[0:1, :] - 1.0, -1.0)
    pos_ref[...] = jnp.broadcast_to(pos, (8, tokens))
    gain = g_ref[...].astype(F32)
    bias = b_ref[...].astype(F32)

    def block(i, _):
        base = pl.multiple_of(i * TB, TB)
        want = (lax.broadcasted_iota(jnp.int32, (TB, tokens), 0) + base).astype(F32)
        pick = jnp.where(want == pos_ref[0:1, :], 1.0, 0.0).astype(BF16)
        h32 = nn(pick, h_ref[...])
        hc_ref[pl.ds(base, TB), :] = h32.astype(BF16)
        xhat, _ = normed(h32)
        x_ref[pl.ds(base, TB), :] = (xhat * gain + bias).astype(BF16).astype(F32)
        parts = nt(table, pick)
        label = jnp.where(parts[2:3, :] > 0.5, parts[0:1, :] * 256.0 + parts[1:2, :], -1.0)
        yc_ref[i] = jnp.broadcast_to(label, (8, TB))
        return 0

    lax.fori_loop(0, tokens // TB, block, 0)


def prep(count, h, mask_label, gain, bias):
    tokens, width = h.shape
    vm = pl.BlockSpec(memory_space=pltpu.VMEM)
    return pl.pallas_call(
        prep_kernel,
        name="prep",
        in_specs=[pl.BlockSpec(memory_space=pltpu.SMEM), vm, vm, vm, vm],
        out_specs=[vm] * 4,
        out_shape=[
            jax.ShapeDtypeStruct((tokens, width), BF16),
            jax.ShapeDtypeStruct((tokens, width), F32),
            jax.ShapeDtypeStruct((8, tokens), F32),
            jax.ShapeDtypeStruct((tokens // TB, 8, TB), F32),
        ],
        compiler_params=pltpu.CompilerParams(vmem_limit_bytes=48 << 20),
        cost_estimate=pl.CostEstimate(flops=2 * tokens * tokens * width, bytes_accessed=10 * tokens * width, transcendentals=0),
    )(count, h, mask_label, gain, bias)


def stat_kernel(rows, chunk, n_ref, x_ref, yc_ref, e_ref, o_ref, xb_ref, m_ref, s_ref, t_ref):
    step = pl.program_id(0)
    blocks = n_ref[0]
    first = n_ref[1] + step * rows

    @pl.when(step == 0)
    def _():
        xb_ref[...] = x_ref[...].astype(BF16)
        m_ref[...] = jnp.full_like(m_ref, LOW)
        s_ref[...] = jnp.zeros_like(s_ref)
        t_ref[...] = jnp.zeros_like(t_ref)

    def body(t, _):
        x = xb_ref[pl.ds(pl.multiple_of(t * TB, TB), TB), :]
        label = yc_ref[t].astype(jnp.int32)[0:1, :]
        m8 = m_ref[t]
        s8 = s_ref[t]
        t8 = t_ref[t]
        for i in range(0, rows, chunk):
            z = nt(e_ref[i : i + chunk, :], x)
            ids = lax.broadcasted_iota(jnp.int32, (chunk, 1), 0) + (first + i)
            z = jnp.where(ids < VOCAB, z, LOW).reshape(chunk // 8, 8, TB)
            hit = (ids == label).reshape(chunk // 8, 8, TB)
            t8 = t8 + jnp.sum(jnp.where(hit, z, 0.0), axis=0)
            new = jnp.maximum(m8, jnp.max(z, axis=0))
            s8 = s8 * jnp.exp2((m8 - new) * LOG2E) + jnp.sum(jnp.exp2((z - new[None]) * LOG2E), axis=0)
            m8 = new
        m_ref[t] = m8
        s_ref[t] = s8
        t_ref[t] = t8
        return 0

    lax.fori_loop(0, blocks, body, 0)

    @pl.when(step == pl.num_programs(0) - 1)
    def _():
        for t in range(m_ref.shape[0]):
            m8 = m_ref[t]
            top = jnp.max(m8, axis=0, keepdims=True)
            total = jnp.sum(s_ref[t] * jnp.exp2((m8 - top) * LOG2E), axis=0, keepdims=True)
            target = jnp.sum(t_ref[t], axis=0, keepdims=True)
            o_ref[:, t * TB : (t + 1) * TB] = jnp.concatenate([top, total, target, yc_ref[t][0:1, :]], axis=0)


def local_stats(scalars, x, yc, table, rows, chunk):
    tokens, width = x.shape
    shard = table.shape[0]
    nb = tokens // TB
    return pl.pallas_call(
        functools.partial(stat_kernel, rows, chunk),
        name="stat",
        grid_spec=pltpu.PrefetchScalarGridSpec(
            num_scalar_prefetch=1,
            grid=(shard // rows,),
            in_specs=[
                pl.BlockSpec((tokens, width), lambda r, n: (0, 0), pipeline_mode=pl.Buffered(1)),
                pl.BlockSpec((nb, 8, TB), lambda r, n: (0, 0, 0), pipeline_mode=pl.Buffered(1)),
                pl.BlockSpec((rows, width), lambda r, n: (r, 0)),
            ],
            out_specs=pl.BlockSpec((4, tokens), lambda r, n: (0, 0)),
            scratch_shapes=[pltpu.VMEM((tokens, width), BF16)] + [pltpu.VMEM((nb, 8, TB), F32)] * 3,
        ),
        out_shape=jax.ShapeDtypeStruct((4, tokens), F32),
        compiler_params=pltpu.CompilerParams(vmem_limit_bytes=48 << 20),
        cost_estimate=pl.CostEstimate(flops=2 * tokens * shard * width // 2, bytes_accessed=2 * shard * width, transcendentals=0),
    )(scalars, x, yc, table)


def join_kernel(shards, groups, st_ref, cy_ref, cnt_ref, loss_ref):
    total = jnp.float32(0.0)
    acc = jnp.float32(0.0)
    for g in range(groups):
        parts = [st_ref[g * shards + j] for j in range(shards)]
        live = parts[0][3:4, :] >= 0.0
        n = jnp.sum(jnp.where(live, 1.0, 0.0))
        cnt_ref[g] = n.astype(jnp.int32)
        total = total + n
    log_total = jnp.log(jnp.full((1, 128), total))[0:1, 0:1]
    for g in range(groups):
        parts = [st_ref[g * shards + j] for j in range(shards)]
        label = parts[0][3:4, :]
        live = label >= 0.0
        top = functools.reduce(jnp.maximum, [p[0:1, :] for p in parts])
        exp_sum = sum(p[1:2, :] * jnp.exp2((p[0:1, :] - top) * LOG2E) for p in parts)
        target = sum(p[2:3, :] for p in parts)
        lse = top + jnp.log(exp_sum)
        acc = acc + jnp.sum(jnp.where(live, lse - target, 0.0))
        c = jnp.where(live, lse + log_total, jnp.inf)
        pad = jnp.zeros((6, c.shape[1]), F32)
        cy_ref[g] = jnp.concatenate([c, label, pad], axis=0)
    cnt_ref[groups] = total.astype(jnp.int32)
    loss_ref[...] = jnp.full((1, 128), acc) / jnp.full((1, 128), total)


def join(stats, shards, groups):
    tokens = stats.shape[-1]
    return pl.pallas_call(
        functools.partial(join_kernel, shards, groups),
        name="join",
        in_specs=[pl.BlockSpec(memory_space=pltpu.VMEM)],
        out_specs=[pl.BlockSpec(memory_space=pltpu.VMEM), pl.BlockSpec(memory_space=pltpu.SMEM), pl.BlockSpec(memory_space=pltpu.VMEM)],
        out_shape=[
            jax.ShapeDtypeStruct((groups, 8, tokens), F32),
            jax.ShapeDtypeStruct((groups + 1,), jnp.int32),
            jax.ShapeDtypeStruct((1, 128), F32),
        ],
        cost_estimate=pl.CostEstimate(flops=1000, bytes_accessed=stats.size * 4, transcendentals=0),
    )(stats)


def dx_kernel(cols, n_ref, inv_ref, x_ref, cy_ref, e_ref, o_ref, xb_ref, cyt_ref):
    step = pl.program_id(0)
    blocks = n_ref[0]
    first = n_ref[1] + step * cols
    inv = inv_ref[0]
    tile = 2 * TB

    @pl.when(step == 0)
    def _():
        xb_ref[...] = x_ref[...].astype(BF16)
        cyt_ref[...] = cy_ref[0].T
        o_ref[...] = jnp.zeros_like(o_ref)

    ids = lax.broadcasted_iota(jnp.int32, (1, cols), 1) + first

    def body(t, _):
        at = pl.ds(pl.multiple_of(t * tile, tile), tile)
        cy = cyt_ref[at, :]
        c = cy[:, 0:1]
        label = cy[:, 1:2].astype(jnp.int32)
        z = nt(xb_ref[at, :], e_ref[...])
        p = jnp.exp2((z - c) * LOG2E) - jnp.where(ids == label, inv, 0.0)
        q = jnp.where(ids < VOCAB, p, 0.0).astype(BF16)
        o_ref[at, :] += nn(q, e_ref[...])
        return 0

    lax.fori_loop(0, blocks, body, 0)


def local_dx(scalars, inv, x, cy, table, cols):
    tokens, width = x.shape
    shard = table.shape[0]
    return pl.pallas_call(
        functools.partial(dx_kernel, cols),
        name="dx",
        grid_spec=pltpu.PrefetchScalarGridSpec(
            num_scalar_prefetch=2,
            grid=(shard // cols,),
            in_specs=[
                pl.BlockSpec((tokens, width), lambda r, n, i: (0, 0), pipeline_mode=pl.Buffered(1)),
                pl.BlockSpec((1, 8, tokens), lambda r, n, i: (n[2], 0, 0), pipeline_mode=pl.Buffered(1)),
                pl.BlockSpec((cols, width), lambda r, n, i: (r, 0)),
            ],
            out_specs=pl.BlockSpec((tokens, width), lambda r, n, i: (0, 0), pipeline_mode=pl.Buffered(1)),
            scratch_shapes=[pltpu.VMEM((tokens, width), BF16), pltpu.VMEM((tokens, 8), F32)],
        ),
        out_shape=jax.ShapeDtypeStruct((tokens, width), F32),
        compiler_params=pltpu.CompilerParams(vmem_limit_bytes=56 << 20),
        cost_estimate=pl.CostEstimate(flops=4 * tokens * shard * width // 2, bytes_accessed=2 * shard * width, transcendentals=0),
    )(scalars, inv, x, cy, table)


ROWS_IN = 128


def de_kernel(rows, chunk, groups, cap, n_ref, inv_ref, cy_ref, x_hbm, e_hbm, o_hbm,
              x_ref, e_ref, acc_ref, q_ref, stage_ref, cyt_ref, cyr_ref, xsem, esem, osem):
    nr = e_hbm.shape[0] // rows
    width = e_hbm.shape[1]
    first_row = n_ref[groups + 1]
    inv = inv_ref[0]
    slots = stage_ref.shape[0]

    def e_copy(r):
        return pltpu.make_async_copy(e_hbm.at[pl.ds(pl.multiple_of(r * rows, 16), rows)], e_ref.at[lax.rem(r, 2)], esem.at[lax.rem(r, 2)])

    def o_copy(r):
        return pltpu.make_async_copy(acc_ref.at[lax.rem(r, 2)], o_hbm.at[pl.ds(pl.multiple_of(r * rows, 16), rows)], osem.at[lax.rem(r, 2)])

    def x_copy(g, k, slot):
        return pltpu.make_async_copy(x_hbm.at[pl.ds(pl.multiple_of(g * cap + k * ROWS_IN, ROWS_IN), ROWS_IN)], stage_ref.at[slot], xsem.at[slot])

    e_copy(0).start()

    def pieces(g):
        return (n_ref[g] + (ROWS_IN - 1)) // ROWS_IN

    def advance(g, k):
        g2, k2 = g, k + 1

        def cond(s):
            return jnp.logical_and(s[0] < groups, s[1] >= pieces(jnp.minimum(s[0], groups - 1)))

        return lax.while_loop(cond, lambda s: (s[0] + 1, jnp.int32(0)), (g2, k2))

    total = jnp.int32(0)
    count = jnp.int32(0)
    for g in range(groups):
        total = total + pieces(g)
        count = count + (n_ref[g] + 15) // 16 * 16
    nb = (count + (TB - 1)) // TB

    start = advance(jnp.int32(0), jnp.int32(-1))

    def prime(i, s):
        @pl.when(i < total)
        def _():
            x_copy(s[0], s[1], i).start()

        return advance(s[0], s[1])

    ahead = lax.fori_loop(0, slots, prime, start)

    def place(i, s):
        g, k, base, ga, ka = s
        slot = lax.rem(i, slots)
        x_copy(g, k, slot).wait()
        x_ref[pl.ds(pl.multiple_of(base + k * ROWS_IN, 16), ROWS_IN), :] = stage_ref[slot].astype(BF16)

        @pl.when(i + slots < total)
        def _():
            x_copy(ga, ka, slot).start()

        ga, ka = advance(ga, ka)
        g2, k2 = advance(g, k)
        def bump(s):
            return s[0] + 1, s[1] + (n_ref[s[0]] + 15) // 16 * 16

        _, base = lax.while_loop(lambda s: s[0] < g2, bump, (g, base))
        return g2, k2, base, ga, ka

    base0 = jnp.int32(0)
    lax.fori_loop(0, total, place, (start[0], start[1], base0, ahead[0], ahead[1]))

    @pl.when(count < nb * TB)
    def _():
        def wipe(i, _):
            at = pl.ds(pl.multiple_of(count + i * 16, 16), 16)
            x_ref[at, :] = jnp.zeros((16, width), BF16)
            return 0

        lax.fori_loop(0, (nb * TB - count) // 16, wipe, 0)

    base = jnp.int32(0)
    for g in range(groups):
        cyt_ref[pl.ds(pl.multiple_of(base, 16), cap), :] = cy_ref[g].T
        base = base + (n_ref[g] + 15) // 16 * 16
    tail = jnp.where(lax.broadcasted_iota(jnp.int32, (TB, 8), 1) == 0, jnp.inf, -1.0)
    cyt_ref[pl.ds(pl.multiple_of(base, 16), TB), :] = tail

    def rows_of(t, _):
        cyr_ref[t] = cyt_ref[pl.ds(pl.multiple_of(t * TB, TB), TB), :].T
        return 0

    lax.fori_loop(0, nb, rows_of, 0)

    steps = nb * nr

    def body(s, carry):
        r, t, rp, tp = carry

        @pl.when(jnp.logical_and(t == 0, s < steps))
        def _():
            e_copy(r).wait()

            @pl.when(r + 1 < nr)
            def _():
                e_copy(r + 1).start()

        @pl.when(jnp.logical_and(jnp.logical_and(tp == 0, s > 0), rp >= 2))
        def _():
            o_copy(rp - 2).wait()

        x = x_ref[pl.ds(pl.multiple_of(t * TB, TB), TB), :]
        xp = x_ref[pl.ds(pl.multiple_of(tp * TB, TB), TB), :]
        c = cyr_ref[t, 0:1, :]
        label = cyr_ref[t, 1:2, :].astype(jnp.int32)
        fresh = tp == 0
        es = lax.rem(r, 2)
        os = lax.rem(rp, 2)
        for i in range(0, rows, chunk):
            d = nn(q_ref[i : i + chunk, :], xp)
            acc_ref[os, i : i + chunk, :] = jnp.where(fresh, 0.0, acc_ref[os, i : i + chunk, :]) + d
            z = nt(e_ref[es, i : i + chunk, :], x)
            ids = lax.broadcasted_iota(jnp.int32, (chunk, 1), 0) + (first_row + r * rows + i)
            p = jnp.exp2((z - c) * LOG2E) - jnp.where(ids == label, inv, 0.0)
            q_ref[i : i + chunk, :] = p.astype(BF16)

        @pl.when(jnp.logical_and(tp == nb - 1, s > 0))
        def _():
            @pl.when(first_row + (rp + 1) * rows > VOCAB)
            def _():
                def clear(i, _):
                    at = pl.ds(pl.multiple_of(i * 16, 16), 16)
                    ids = lax.broadcasted_iota(jnp.int32, (16, 1), 0) + (first_row + rp * rows + i * 16)
                    acc_ref[os, at, :] = jnp.where(ids < VOCAB, acc_ref[os, at, :], 0.0)
                    return 0

                lax.fori_loop(0, rows // 16, clear, 0)

            o_copy(rp).start()

        more = t + 1
        wrap = more == nb
        return jnp.where(wrap, jnp.minimum(r + 1, nr - 1), r), jnp.where(wrap, 0, more), r, t

    zero = jnp.int32(0)
    lax.fori_loop(0, steps + 1, body, (zero, zero, zero, zero))
    if nr > 1:
        o_copy(nr - 2).wait()
    o_copy(nr - 1).wait()


def vocab_grad(scalars, inv, cy, x_all, table, rows, chunk, groups):
    width = table.shape[1]
    shard = table.shape[0]
    cap = x_all.shape[0] // groups
    most = groups * cap + TB
    any_ = pl.BlockSpec(memory_space=pl.ANY)
    smem = pl.BlockSpec(memory_space=pltpu.SMEM)
    return pl.pallas_call(
        functools.partial(de_kernel, rows, chunk, groups, cap),
        name="grad",
        in_specs=[smem, smem, pl.BlockSpec(memory_space=pltpu.VMEM), any_, any_],
        out_specs=any_,
        out_shape=jax.ShapeDtypeStruct((shard, width), F32),
        scratch_shapes=[
            pltpu.VMEM((most, width), BF16),
            pltpu.VMEM((2, rows, width), BF16),
            pltpu.VMEM((2, rows, width), F32),
            pltpu.VMEM((rows, TB), BF16),
            pltpu.VMEM((4, ROWS_IN, width), F32),
            pltpu.VMEM((most + cap, 8), F32),
            pltpu.VMEM((most // TB, 8, TB), F32),
            pltpu.SemaphoreType.DMA((4,)),
            pltpu.SemaphoreType.DMA((2,)),
            pltpu.SemaphoreType.DMA((2,)),
        ],
        compiler_params=pltpu.CompilerParams(vmem_limit_bytes=VMEM_MAX),
        cost_estimate=pl.CostEstimate(flops=4 * groups * cap * shard * width // 2, bytes_accessed=6 * shard * width, transcendentals=0),
    )(scalars, inv, cy, x_all, table)


def back_kernel(dx_ref, hc_ref, pos_ref, g_ref, dh_ref, dg_ref, db_ref, dhc_ref, post_ref):
    tokens, width = hc_ref.shape
    gain = g_ref[...].astype(F32)
    dg_ref[...] = jnp.zeros_like(dg_ref)
    db_ref[...] = jnp.zeros_like(db_ref)
    post_ref[...] = pos_ref[...].T

    def block(i, _):
        at = pl.ds(pl.multiple_of(i * TB, TB), TB)
        xhat, inv_std = normed(hc_ref[at, :].astype(F32))
        dx = dx_ref[at, :]
        dg_ref[...] += jnp.sum((dx * xhat).reshape(TB // 8, 8, width), axis=0)
        db_ref[...] += jnp.sum(dx.reshape(TB // 8, 8, width), axis=0)
        u = dx * gain
        mean_u = jnp.mean(u, axis=-1, keepdims=True)
        mean_p = jnp.mean(u * xhat, axis=-1, keepdims=True)
        dhc_ref[at, :] = (inv_std * (u - mean_u - xhat * mean_p)).astype(BF16)
        return 0

    lax.fori_loop(0, tokens // TB, block, 0)

    def spread(i, _):
        at = pl.ds(pl.multiple_of(i * TB, TB), TB)
        slot = lax.broadcasted_iota(jnp.int32, (TB, tokens), 1).astype(F32)
        pick = jnp.where(slot == post_ref[at, 0:1], 1.0, 0.0).astype(BF16)
        dh_ref[at, :] = nn(pick, dhc_ref[...]).astype(BF16)
        return 0

    lax.fori_loop(0, tokens // TB, spread, 0)


def back(dx, hc, pos, gain):
    tokens, width = hc.shape
    vm = pl.BlockSpec(memory_space=pltpu.VMEM)
    return pl.pallas_call(
        back_kernel,
        name="back",
        in_specs=[vm] * 4,
        out_specs=[vm] * 3,
        out_shape=[
            jax.ShapeDtypeStruct((tokens, width), BF16),
            jax.ShapeDtypeStruct((8, width), F32),
            jax.ShapeDtypeStruct((8, width), F32),
        ],
        scratch_shapes=[pltpu.VMEM((tokens, width), BF16), pltpu.VMEM((tokens, 8), F32)],
        compiler_params=pltpu.CompilerParams(vmem_limit_bytes=48 << 20),
        cost_estimate=pl.CostEstimate(flops=2 * tokens * tokens * width, bytes_accessed=10 * tokens * width, transcendentals=0),
    )(dx, hc, pos, gain)


SIZES = dict(stat_rows=3264, stat_chunk=272, dx_cols=768, de_rows=3264, de_chunk=272)


def solution(mesh):
    shards = mesh.shape["tp"]
    groups = mesh.shape["dp"]

    def device_step(hidden, table, labels, loss_mask, ln_gain, ln_bias):
        batch, seq, width = hidden.shape
        tokens = batch * seq
        shard = table.shape[0]
        me = lax.axis_index("tp")
        group = lax.axis_index("dp")
        first = me * shard
        h = hidden.reshape(tokens, width)
        mask = loss_mask.reshape(1, tokens)
        mask_label = jnp.concatenate([mask, labels.reshape(1, tokens)] + [jnp.zeros((6, tokens), jnp.int32)], axis=0).astype(F32)
        count = jnp.sum(mask)
        hc, x, pos, yc = prep(count.reshape(1), h, mask_label, ln_gain.reshape(1, width), ln_bias.reshape(1, width))
        part = tokens // shards
        x_all = lax.all_gather(lax.dynamic_slice_in_dim(x, me * part, part), ("dp", "tp"), tiled=True)
        stats = local_stats(jnp.stack([(count + TB - 1) // TB, first]), x, yc, table, SIZES["stat_rows"], SIZES["stat_chunk"])
        stats = lax.all_gather(stats, ("dp", "tp"))
        cy, counts, loss = join(stats, shards, groups)
        inv = (1.0 / counts[groups].astype(F32)).reshape(1)
        dx = local_dx(jnp.stack([(count + 2 * TB - 1) // (2 * TB), first, group]), inv, x, cy, table, SIZES["dx_cols"])
        dx = lax.psum(dx, "tp")
        scalars = jnp.concatenate([counts, first.reshape(1)])
        grad_table = vocab_grad(scalars, inv, cy, x_all, table, SIZES["de_rows"], SIZES["de_chunk"], groups)
        dh, dg, db = back(dx, hc, pos, ln_gain.reshape(1, width))
        sums = lax.psum(jnp.stack([jnp.sum(dg, axis=0), jnp.sum(db, axis=0)]), "dp")
        return loss[0, 0], dh.reshape(batch, seq, width), grad_table, sums[0], sums[1]

    specs_in = (P("dp", None, None), P("tp", None), P("dp", None), P("dp", None), P(None), P(None))
    specs_out = (P(), P("dp", None, None), P("tp", None), P(None), P(None))
    return jax.shard_map(device_step, mesh=mesh, in_specs=specs_in, out_specs=specs_out, check_vma=False)
```
